32 devices in a mesh: seq: 8 (over z, y), tp: 4 (over x, core).
Axes of the slice: x: 2, y: 2, z: 4, core: 2. Of those that a mesh axis runs over, the one named last changes fastest.
Arguments:
- inputs: bfloat16 [2, 32, 8192], P(None, 'seq', 'tp'), may hold values from -6 to 6
- out_grad: bfloat16 [2, 32, 8192], P(None, 'seq', 'tp'), may hold values from -6 to 6
- gate_weight: bfloat16 [8192, 14848], P('tp', 'seq'), may hold values from -0.0625 to 0.0625
- up_weight: bfloat16 [8192, 14848], P('tp', 'seq'), may hold values from -0.0625 to 0.0625
- down_weight: bfloat16 [14848, 8192], P('seq', 'tp'), may hold values from -0.0625 to 0.0625
Outputs:
- input_grad: bfloat16 [2, 32, 8192], P(None, 'seq', 'tp')
- gate_grad: float32 [8192, 14848], P('tp', 'seq')
- up_grad: float32 [8192, 14848], P('tp', 'seq')
- down_grad: float32 [14848, 8192], P('seq', 'tp')
The draws below stay inside these ranges and needn't reach their ends.
All inputs are finite; a program needn't handle non-finite values.
Results may differ from the reference program's by a relative error of at most 0.0049.
Values may be sent and summed in bfloat16 or wider, within the bound.
A program may use at most 128 MiB of HBM per device.

```python
import jax
import jax.numpy as jnp

D = 8192
FFW = 14848
GROUPS = 2
TC = 32


def steps_of(rng, shape, pieces, least, high):
    factor_of = 1.0
    for axis_at, shards_of in pieces:
        draws = jax.random.uniform(jax.random.fold_in(jax.random.fold_in(rng, 6), axis_at), (shards_of,), jnp.float32, least / len(pieces), high / len(pieces))
        factor_of = factor_of * jnp.repeat(jnp.exp(draws), shape[axis_at] // shards_of).reshape((-1,) + (1,) * (len(shape) - 1 - axis_at))
    return factor_of


def normal_values(own_key, dims, scale, bound, shards=(), kind=jnp.bfloat16):
    array = jax.random.normal(own_key, dims, jnp.float32) * scale
    if len(shards) > 0:
        array = steps_of(own_key, dims, shards, -0.22, 0.18) * array
    return jnp.clip(array, min=-bound, max=bound).astype(kind)


def setup_inputs(seed: int = 0) -> dict:
    key_of = jax.random.split(jax.random.key(seed), 6)
    return {
        "inputs": normal_values(key_of[0], (GROUPS, TC, D), 1.0, 6.0, ((1, 8), (2, 4))),
        "out_grad": normal_values(key_of[1], (GROUPS, TC, D), 1.0, 6.0, ((1, 8), (2, 4))),
        "gate_weight": normal_values(key_of[2], (D, FFW), D ** -0.5, 0.0625, ((0, 4), (1, 8))),
        "up_weight": normal_values(key_of[3], (D, FFW), D ** -0.5, 0.0625, ((0, 4), (1, 8))),
        "down_weight": normal_values(key_of[4], (FFW, D), D ** -0.5, 0.0625, ((0, 8), (1, 4))),
    }


def reference(inputs, out_grad, gate_weight, up_weight, down_weight):
    gate_total = jnp.zeros((D, FFW), jnp.float32)
    up_total = jnp.zeros((D, FFW), jnp.float32)
    down_total = jnp.zeros((FFW, D), jnp.float32)
    results = []
    for index in range(GROUPS):
        block_in = inputs[index]
        block_grad = out_grad[index]
        gate = jnp.dot(block_in, gate_weight, preferred_element_type=jnp.float32)
        up_proj = jnp.dot(block_in, up_weight, preferred_element_type=jnp.float32)
        hidden = (jax.nn.silu(gate) * up_proj).astype(jnp.bfloat16)
        hidden_grad = jnp.dot(block_grad, down_weight.T, preferred_element_type=jnp.float32)
        sig = jax.nn.sigmoid(gate)
        up_unit = (hidden_grad * gate * sig).astype(jnp.bfloat16)
        gate_unit = (hidden_grad * up_proj * sig * (1.0 + gate * (1.0 - sig))).astype(jnp.bfloat16)
        grad_in = jnp.dot(gate_unit, gate_weight.T, preferred_element_type=jnp.float32)
        grad_in = grad_in + jnp.dot(up_unit, up_weight.T, preferred_element_type=jnp.float32)
        results.append(grad_in.astype(jnp.bfloat16))
        gate_total = gate_total + jnp.dot(block_in.T, gate_unit, preferred_element_type=jnp.float32)
        up_total = up_total + jnp.dot(block_in.T, up_unit, preferred_element_type=jnp.float32)
        down_total = down_total + jnp.dot(hidden.T, block_grad, preferred_element_type=jnp.float32)
    return jnp.stack(results), gate_total, up_total, down_total
```

```python
import functools

import jax
import jax.numpy as jnp
from jax import lax
from jax.experimental import pallas as pl
from jax.experimental.pallas import tpu as pltpu
from jax.sharding import PartitionSpec as P

MESH = pl.DeviceIdType.MESH
F32 = jnp.float32
BF16 = jnp.bfloat16
NT = (((1,), (1,)), ((), ()))
TILE = 256
ROWS = 128


def tiles_of(size, tile, body):
    whole = size // tile

    @pl.loop(0, whole)
    def _(i):
        body(pl.multiple_of(i * tile, tile), tile)

    if size % tile:
        body(whole * tile, size % tile)


def front_kernel(n_seq, n_tp, x_ref, dy_ref, wg_hbm, wu_hbm, wd_hbm,
                 x_out, dy_out, hid_out, gu_out, uu_out, ig_out,
                 gath, wg, wu, wd, part, from_core, chip_sum, sendx, from_chip, acts,
                 w_sem, z_send, z_recv, y_send, y_recv,
                 c_send, c_recv, r_send, r_recv, a_send, a_recv, f_send, f_recv):
    seq = lax.axis_index("seq")
    tp = lax.axis_index("tp")
    nz, nchip = n_seq // 2, n_tp // 2
    z, y = seq // 2, lax.rem(seq, 2)
    chip, core = tp // 2, lax.rem(tp, 2)
    tokens, ffw = hid_out.shape
    share = tokens // n_tp
    at_y = {"seq": z * 2 + (1 - y)}
    at_core = {"tp": chip * 2 + (1 - core)}

    def z_at(k):
        return lax.rem(z + k, nz)

    def chip_at(k):
        return lax.rem(chip + k, nchip)

    loads = [
        pltpu.make_async_copy(src, dst, w_sem.at[i])
        for i, (src, dst) in enumerate(((wg_hbm, wg), (wu_hbm, wu), (wd_hbm, wd)))
    ]
    for load in loads:
        load.start()

    barrier = pltpu.get_barrier_semaphore()
    for k in range(1, nz):
        pl.semaphore_signal(barrier, inc=1, device_id={"seq": z_at(k) * 2 + y}, device_id_type=MESH)
    for k in range(1, nchip):
        pl.semaphore_signal(barrier, inc=1, device_id={"tp": chip_at(k) * 2 + core}, device_id_type=MESH)
    pl.semaphore_signal(barrier, inc=1, device_id=at_y, device_id_type=MESH)
    pl.semaphore_signal(barrier, inc=1, device_id=at_core, device_id_type=MESH)
    pl.semaphore_wait(barrier, nz - 1 + nchip - 1 + 2)

    def remote(src, dst, send, recv, to):
        return pltpu.make_async_remote_copy(
            src_ref=src, dst_ref=dst, send_sem=send, recv_sem=recv, device_id=to, device_id_type=MESH
        )

    z_copies, y_copies = [], []
    for a, ref in enumerate((x_ref, dy_ref)):
        own = [
            remote(ref, gath.at[a, z, y], z_send.at[a, k], z_recv.at[a, k], {"seq": z_at(k) * 2 + y})
            for k in range(1, nz)
        ]
        over = [remote(ref, gath.at[a, z, y], y_send.at[a, 0], y_recv.at[a, 0], at_y)]
        over += [
            remote(gath.at[a, z_at(nz - k), y], gath.at[a, z_at(nz - k), y],
                   y_send.at[a, k], y_recv.at[a, k], at_y)
            for k in range(1, nz)
        ]
        z_copies.append(own)
        y_copies.append(over)
    for a in range(2):
        y_copies[a][0].start()
        for copy in z_copies[a]:
            copy.start()
    for a, ref in enumerate((x_ref, dy_ref)):
        gath[a, z, y] = ref[...]

    def forward(a):
        for k in range(1, nz):
            z_copies[a][k - 1].wait_recv()
            y_copies[a][k].start()

    def arrive(a, out):
        for k in range(nz):
            y_copies[a][k].wait_recv()
        out[...] = gath[a].astype(F32).reshape(out.shape).astype(BF16)

    c_copies = [
        remote(part.at[q, :, 1 - core], from_core.at[q], c_send.at[q], c_recv.at[q], at_core)
        for q in range(3)
    ]
    r_copies = [
        [
            remote(sendx.at[q, k - 1], from_chip.at[q, k - 1], r_send.at[q, k], r_recv.at[q, k],
                   {"tp": chip_at(k) * 2 + core})
            for k in range(1, nchip)
        ]
        for q in range(3)
    ]

    def product(q, out, w, last):
        def body(start, width):
            if last:
                val = lax.dot_general(out[...], w[pl.ds(start, width), :], NT, preferred_element_type=F32)
            else:
                val = jnp.dot(out[...], w[:, pl.ds(start, width)], preferred_element_type=F32)
            part[q, :, :, :, pl.ds(start, width)] = val.reshape(nchip, 2, share, width)

        tiles_of(ffw, TILE, body)
        c_copies[q].start()

    def reduce_chip(q):
        c_copies[q].wait_recv()
        for k in range(1, nchip):
            sendx[q, k - 1] = (part[q, chip_at(k), core] + from_core[q, chip_at(k)]).astype(BF16)
            r_copies[q][k - 1].start()
        chip_sum[q] = part[q, chip, core] + from_core[q, chip]

    forward(0)
    arrive(0, x_out)
    loads[0].wait()
    product(0, x_out, wg, False)
    forward(1)
    loads[1].wait()
    product(1, x_out, wu, False)
    reduce_chip(0)
    reduce_chip(1)
    arrive(1, dy_out)
    loads[2].wait()
    product(2, dy_out, wd, True)
    reduce_chip(2)
    for q in range(3):
        for k in range(1, nchip):
            r_copies[q][k - 1].wait_recv()

    def total(q):
        value = chip_sum[q]
        for k in range(1, nchip):
            value = value + from_chip[q, k - 1].astype(F32)
        return value

    gate, up, grad = total(0), total(1), total(2)
    sig = jax.nn.sigmoid(gate)
    acts[0, chip, core] = (grad * up * sig * (1.0 + gate * (1.0 - sig))).astype(BF16)
    acts[1, chip, core] = (grad * gate * sig).astype(BF16)
    acts[2, chip, core] = (gate * sig * up).astype(BF16)

    a_copies, f_copies = [], []
    for q in range(3):
        mine = acts.at[q, chip, core]
        a_copies.append([
            remote(mine, mine, a_send.at[q, k], a_recv.at[q, k], {"tp": chip_at(k) * 2 + core})
            for k in range(1, nchip)
        ])
        over = [remote(mine, mine, f_send.at[q, 0], f_recv.at[q, 0], at_core)]
        for k in range(1, nchip):
            theirs = acts.at[q, chip_at(nchip - k), core]
            over.append(remote(theirs, theirs, f_send.at[q, k], f_recv.at[q, k], at_core))
        f_copies.append(over)
    for q in range(3):
        for copy in a_copies[q]:
            copy.start()
        f_copies[q][0].start()
    outs = (gu_out, uu_out, hid_out)

    def settle(q):
        for k in range(1, nchip):
            a_copies[q][k - 1].wait_recv()
            f_copies[q][k].start()

    def collect(q):
        for k in range(nchip):
            f_copies[q][k].wait_recv()
        outs[q][...] = acts[q].reshape(tokens, ffw)

    def back(q, w):
        def body(start, width):
            val = lax.dot_general(outs[q][...], w[pl.ds(start, width), :], NT, preferred_element_type=F32)
            if q:
                val = val + ig_out[:, pl.ds(start, width)]
            ig_out[:, pl.ds(start, width)] = val

        tiles_of(ig_out.shape[1], TILE, body)

    settle(0)
    settle(1)
    collect(0)
    back(0, wg)
    settle(2)
    collect(1)
    back(1, wu)
    collect(2)

    for a in range(2):
        for copy in z_copies[a] + y_copies[a]:
            copy.wait_send()
    for q in range(3):
        for copy in [c_copies[q]] + r_copies[q] + a_copies[q] + f_copies[q]:
            copy.wait_send()


def front(n_seq, n_tp, x, dy, wg, wu, wd):
    rows, width = x.shape
    ffw = wg.shape[1]
    tokens = rows * n_seq
    nz, nchip = n_seq // 2, n_tp // 2
    share = tokens // n_tp
    vmem = pl.BlockSpec(memory_space=pltpu.VMEM)
    hbm = pl.BlockSpec(memory_space=pl.ANY)
    dma = pltpu.SemaphoreType.DMA
    others = max(nchip - 1, 1)
    return pl.pallas_call(
        functools.partial(front_kernel, n_seq, n_tp),
        out_shape=[jax.ShapeDtypeStruct((tokens, width), BF16)] * 2
        + [jax.ShapeDtypeStruct((tokens, ffw), BF16)] * 3
        + [jax.ShapeDtypeStruct((tokens, width), F32)],
        in_specs=[vmem, vmem, hbm, hbm, hbm],
        out_specs=[vmem] * 6,
        scratch_shapes=[
            pltpu.VMEM((2, nz, 2, rows, width), BF16),
            pltpu.VMEM(wg.shape, BF16),
            pltpu.VMEM(wu.shape, BF16),
            pltpu.VMEM(wd.shape, BF16),
            pltpu.VMEM((3, nchip, 2, share, ffw), F32),
            pltpu.VMEM((3, nchip, share, ffw), F32),
            pltpu.VMEM((3, share, ffw), F32),
            pltpu.VMEM((3, others, share, ffw), BF16),
            pltpu.VMEM((3, others, share, ffw), BF16),
            pltpu.VMEM((3, nchip, 2, share, ffw), BF16),
            dma((3,)),
            dma((2, nz)), dma((2, nz)), dma((2, nz)), dma((2, nz)),
            dma((3,)), dma((3,)),
            dma((3, nchip)), dma((3, nchip)),
            dma((3, nchip)), dma((3, nchip)), dma((3, nchip)), dma((3, nchip)),
        ],
        compiler_params=pltpu.CompilerParams(
            collective_id=0, has_side_effects=True, vmem_limit_bytes=48 * 1024 * 1024
        ),
        cost_estimate=pl.CostEstimate(
            flops=10 * tokens * width * ffw, bytes_accessed=6 * width * ffw, transcendentals=0
        ),
    )(x, dy, wg, wu, wd)


def weight_kernel(pairs, *refs):
    lefts, rights, outs = refs[:pairs], refs[pairs : 2 * pairs], refs[2 * pairs :]
    for left, right, out in zip(lefts, rights, outs):
        turn = left[...].astype(F32).T.astype(BF16)
        out[...] = jnp.dot(turn, right[...], preferred_element_type=F32)


def weight_grads(left, rights):
    tokens, rows = left.shape
    pairs = len(rights)
    steps = pl.cdiv(rows, ROWS)
    return pl.pallas_call(
        functools.partial(weight_kernel, pairs),
        grid=(steps,),
        out_shape=[jax.ShapeDtypeStruct((rows, right.shape[1]), F32) for right in rights],
        in_specs=[pl.BlockSpec((tokens, ROWS), lambda i: (0, i))] * pairs
        + [pl.BlockSpec(right.shape, lambda i: (0, 0)) for right in rights],
        out_specs=[pl.BlockSpec((ROWS, right.shape[1]), lambda i: (i, 0)) for right in rights],
        cost_estimate=pl.CostEstimate(
            flops=2 * tokens * rows * sum(right.shape[1] for right in rights),
            bytes_accessed=4 * rows * sum(right.shape[1] for right in rights),
            transcendentals=0,
        ),
    )(*([left] * pairs), *rights)


def scatter_sum(n_seq, partial):
    nz = n_seq // 2
    seq = lax.axis_index("seq")
    z, y = seq // 2, lax.rem(seq, 2)
    rows = partial.shape[0] // n_seq
    pieces = partial.reshape(nz, 2, rows, partial.shape[1])
    away = lax.dynamic_index_in_dim(pieces, 1 - y, 1, keepdims=False)
    kept = lax.dynamic_index_in_dim(pieces, y, 1, keepdims=False)
    summed = kept + lax.ppermute(away, "seq", [(i, i ^ 1) for i in range(n_seq)])
    result = lax.dynamic_index_in_dim(summed, z, 0, keepdims=False)
    for k in range(1, nz):
        send = lax.dynamic_index_in_dim(summed, lax.rem(z + k, nz), 0, keepdims=False)
        result = result + lax.ppermute(
            send, "seq", [(i, (i + 2 * k) % n_seq) for i in range(n_seq)]
        )
    return result


def solution(mesh):
    n_seq, n_tp = mesh.shape["seq"], mesh.shape["tp"]

    def per_device(inputs, out_grad, gate_weight, up_weight, down_weight):
        blocks, rows, width = inputs.shape
        x, dy, hidden, gate_unit, up_unit, partial = front(
            n_seq, n_tp,
            inputs.reshape(blocks * rows, width), out_grad.reshape(blocks * rows, width),
            gate_weight, up_weight, down_weight,
        )
        gate_grad, up_grad = weight_grads(x, (gate_unit, up_unit))
        (down_grad,) = weight_grads(hidden, (dy,))
        input_grad = scatter_sum(n_seq, partial).astype(BF16).reshape(inputs.shape)
        return input_grad, gate_grad, up_grad, down_grad

    return jax.shard_map(
        per_device,
        mesh=mesh,
        in_specs=(
            P(None, "seq", "tp"),
            P(None, "seq", "tp"),
            P("tp", "seq"),
            P("tp", "seq"),
            P("seq", "tp"),
        ),
        out_specs=(P(None, "seq", "tp"), P("tp", "seq"), P("tp", "seq"), P("seq", "tp")),
        check_vma=False,
    )
```

```python
import functools

import jax
import jax.numpy as jnp
from jax import lax
from jax.experimental import pallas as pl
from jax.experimental.pallas import tpu as pltpu
from jax.sharding import PartitionSpec as P

MESH = pl.DeviceIdType.MESH
F32 = jnp.float32
BF16 = jnp.bfloat16
NT = (((1,), (1,)), ((), ()))
TILE = 256


def tiles_of(size, tile, body):
    whole = size // tile

    @pl.loop(0, whole)
    def _(i):
        body(pl.multiple_of(i * tile, tile), tile)

    if size % tile:
        body(whole * tile, size % tile)


def front_kernel(n_seq, n_tp, x_ref, dy_ref, wg_hbm, wu_hbm, wd_hbm,
                 x_out, dy_out, hid_out, gu_out, uu_out, ig_out,
                 gath, wg, wu, wd, part, from_core, chip_sum, sendx, from_chip, acts,
                 w_sem, z_send, z_recv, y_send, y_recv,
                 c_send, c_recv, r_send, r_recv, a_send, a_recv, f_send, f_recv):
    seq = lax.axis_index("seq")
    tp = lax.axis_index("tp")
    nz, nchip = n_seq // 2, n_tp // 2
    z, y = seq // 2, lax.rem(seq, 2)
    chip, core = tp // 2, lax.rem(tp, 2)
    tokens = hid_out.shape[0]
    ffw = wg_hbm.shape[0]
    share = tokens // n_tp
    at_y = {"seq": z * 2 + (1 - y)}
    at_core = {"tp": chip * 2 + (1 - core)}

    def z_at(k):
        return lax.rem(z + k, nz)

    def chip_at(k):
        return lax.rem(chip + k, nchip)

    loads = [
        pltpu.make_async_copy(src, dst, w_sem.at[i])
        for i, (src, dst) in enumerate(((wg_hbm, wg), (wu_hbm, wu), (wd_hbm, wd)))
    ]
    for load in loads:
        load.start()

    barrier = pltpu.get_barrier_semaphore()
    for k in range(1, nz):
        pl.semaphore_signal(barrier, inc=1, device_id={"seq": z_at(k) * 2 + y}, device_id_type=MESH)
    for k in range(1, nchip):
        pl.semaphore_signal(barrier, inc=1, device_id={"tp": chip_at(k) * 2 + core}, device_id_type=MESH)
    pl.semaphore_signal(barrier, inc=1, device_id=at_y, device_id_type=MESH)
    pl.semaphore_signal(barrier, inc=1, device_id=at_core, device_id_type=MESH)
    pl.semaphore_wait(barrier, nz - 1 + nchip - 1 + 2)

    def remote(src, dst, send, recv, to):
        return pltpu.make_async_remote_copy(
            src_ref=src, dst_ref=dst, send_sem=send, recv_sem=recv, device_id=to, device_id_type=MESH
        )

    z_copies, y_copies = [], []
    for a, ref in enumerate((x_ref, dy_ref)):
        own = [
            remote(ref, gath.at[a, z, y], z_send.at[a, k], z_recv.at[a, k], {"seq": z_at(k) * 2 + y})
            for k in range(1, nz)
        ]
        over = [remote(ref, gath.at[a, z, y], y_send.at[a, 0], y_recv.at[a, 0], at_y)]
        over += [
            remote(gath.at[a, z_at(nz - k), y], gath.at[a, z_at(nz - k), y],
                   y_send.at[a, k], y_recv.at[a, k], at_y)
            for k in range(1, nz)
        ]
        z_copies.append(own)
        y_copies.append(over)
    for a in range(2):
        y_copies[a][0].start()
        for copy in z_copies[a]:
            copy.start()
    for a, ref in enumerate((x_ref, dy_ref)):
        gath[a, z, y] = ref[...]

    def forward(a):
        for k in range(1, nz):
            z_copies[a][k - 1].wait_recv()
            y_copies[a][k].start()

    def arrive(a, out):
        for k in range(nz):
            y_copies[a][k].wait_recv()
        out[...] = gath[a].astype(F32).reshape(out.shape).astype(BF16)

    c_copies = [
        remote(part.at[q, :, 1 - core], from_core.at[q], c_send.at[q], c_recv.at[q], at_core)
        for q in range(3)
    ]
    r_copies = [
        [
            remote(sendx.at[q, k - 1], from_chip.at[q, k - 1], r_send.at[q, k], r_recv.at[q, k],
                   {"tp": chip_at(k) * 2 + core})
            for k in range(1, nchip)
        ]
        for q in range(3)
    ]

    def product(q, out, w):
        def body(start, width):
            val = lax.dot_general(out[...], w[pl.ds(start, width), :], NT, preferred_element_type=F32)
            part[q, :, :, :, pl.ds(start, width)] = val.reshape(nchip, 2, share, width)

        tiles_of(ffw, TILE, body)
        c_copies[q].start()

    def reduce_chip(q):
        c_copies[q].wait_recv()
        for k in range(1, nchip):
            sendx[q, k - 1] = (part[q, chip_at(k), core] + from_core[q, chip_at(k)]).astype(BF16)
            r_copies[q][k - 1].start()
        chip_sum[q] = part[q, chip, core] + from_core[q, chip]

    forward(0)
    arrive(0, x_out)
    loads[0].wait()
    product(0, x_out, wg)
    forward(1)
    loads[1].wait()
    product(1, x_out, wu)
    reduce_chip(0)
    reduce_chip(1)
    arrive(1, dy_out)
    loads[2].wait()
    product(2, dy_out, wd)
    reduce_chip(2)
    for q in range(3):
        for k in range(1, nchip):
            r_copies[q][k - 1].wait_recv()

    def total(q):
        value = chip_sum[q]
        for k in range(1, nchip):
            value = value + from_chip[q, k - 1].astype(F32)
        return value

    gate, up, grad = total(0), total(1), total(2)
    sig = jax.nn.sigmoid(gate)
    acts[0, chip, core] = (grad * up * sig * (1.0 + gate * (1.0 - sig))).astype(BF16)
    acts[1, chip, core] = (grad * gate * sig).astype(BF16)
    acts[2, chip, core] = (gate * sig * up).astype(BF16)

    a_copies, f_copies = [], []
    for q in range(3):
        mine = acts.at[q, chip, core]
        a_copies.append([
            remote(mine, mine, a_send.at[q, k], a_recv.at[q, k], {"tp": chip_at(k) * 2 + core})
            for k in range(1, nchip)
        ])
        over = [remote(mine, mine, f_send.at[q, 0], f_recv.at[q, 0], at_core)]
        for k in range(1, nchip):
            theirs = acts.at[q, chip_at(nchip - k), core]
            over.append(remote(theirs, theirs, f_send.at[q, k], f_recv.at[q, k], at_core))
        f_copies.append(over)
    for q in range(3):
        for copy in a_copies[q]:
            copy.start()
        f_copies[q][0].start()
    outs = (gu_out, uu_out, hid_out)

    def settle(q):
        for k in range(1, nchip):
            a_copies[q][k - 1].wait_recv()
            f_copies[q][k].start()

    def collect(q):
        for k in range(nchip):
            f_copies[q][k].wait_recv()
        if outs[q].shape[1] > ffw:
            start = ffw // 128 * 128
            outs[q][:, start:] = jnp.zeros((tokens, outs[q].shape[1] - start), BF16)
        outs[q][:, :ffw] = acts[q].reshape(tokens, ffw)

    def back(q, w):
        def body(start, width):
            val = jnp.dot(outs[q][:, :ffw], w[:, pl.ds(start, width)], preferred_element_type=F32)
            if q:
                val = val + ig_out[:, pl.ds(start, width)]
            ig_out[:, pl.ds(start, width)] = val

        tiles_of(ig_out.shape[1], TILE, body)

    settle(0)
    settle(1)
    collect(0)
    back(0, wg)
    settle(2)
    collect(1)
    back(1, wu)
    collect(2)

    for a in range(2):
        for copy in z_copies[a] + y_copies[a]:
            copy.wait_send()
    for q in range(3):
        for copy in [c_copies[q]] + r_copies[q] + a_copies[q] + f_copies[q]:
            copy.wait_send()


def front(n_seq, n_tp, x, dy, wg, wu, wd):
    rows, width = x.shape
    ffw = wg.shape[0]
    padded = pl.cdiv(ffw, TILE) * TILE
    tokens = rows * n_seq
    nz, nchip = n_seq // 2, n_tp // 2
    share = tokens // n_tp
    vmem = pl.BlockSpec(memory_space=pltpu.VMEM)
    hbm = pl.BlockSpec(memory_space=pl.ANY)
    dma = pltpu.SemaphoreType.DMA
    others = max(nchip - 1, 1)
    return pl.pallas_call(
        functools.partial(front_kernel, n_seq, n_tp),
        out_shape=[jax.ShapeDtypeStruct((tokens, width), BF16)] * 2
        + [jax.ShapeDtypeStruct((tokens, padded), BF16)] * 3
        + [jax.ShapeDtypeStruct((tokens, width), F32)],
        in_specs=[vmem, vmem, hbm, hbm, hbm],
        out_specs=[vmem] * 6,
        scratch_shapes=[
            pltpu.VMEM((2, nz, 2, rows, width), BF16),
            pltpu.VMEM(wg.shape, BF16),
            pltpu.VMEM(wu.shape, BF16),
            pltpu.VMEM(wd.shape, BF16),
            pltpu.VMEM((3, nchip, 2, share, ffw), F32),
            pltpu.VMEM((3, nchip, share, ffw), F32),
            pltpu.VMEM((3, share, ffw), F32),
            pltpu.VMEM((3, others, share, ffw), BF16),
            pltpu.VMEM((3, others, share, ffw), BF16),
            pltpu.VMEM((3, nchip, 2, share, ffw), BF16),
            dma((3,)),
            dma((2, nz)), dma((2, nz)), dma((2, nz)), dma((2, nz)),
            dma((3,)), dma((3,)),
            dma((3, nchip)), dma((3, nchip)),
            dma((3, nchip)), dma((3, nchip)), dma((3, nchip)), dma((3, nchip)),
        ],
        compiler_params=pltpu.CompilerParams(
            collective_id=0, has_side_effects=True, vmem_limit_bytes=48 * 1024 * 1024
        ),
        cost_estimate=pl.CostEstimate(
            flops=10 * tokens * width * ffw, bytes_accessed=6 * width * ffw, transcendentals=0
        ),
    )(x, dy, wg, wu, wd)


def weight_kernel(pairs, *refs):
    lefts, right, outs = refs[:pairs], refs[pairs], refs[pairs + 1 :]
    columns = pl.ds(pl.multiple_of(pl.program_id(0) * TILE, TILE), TILE)
    for left, out in zip(lefts, outs):
        turned = left[:, columns].astype(F32).T.astype(BF16)
        out[...] = jnp.dot(turned, right[...], preferred_element_type=F32)


def weight_grads(rows, lefts, right):
    tokens, width = right.shape
    pairs = len(lefts)
    return pl.pallas_call(
        functools.partial(weight_kernel, pairs),
        grid=(pl.cdiv(rows, TILE),),
        out_shape=[jax.ShapeDtypeStruct((rows, width), F32)] * pairs,
        in_specs=[pl.BlockSpec(memory_space=pltpu.VMEM)] * (pairs + 1),
        out_specs=[pl.BlockSpec((TILE, width), lambda i: (i, 0))] * pairs,
        cost_estimate=pl.CostEstimate(
            flops=2 * pairs * tokens * rows * width,
            bytes_accessed=4 * pairs * rows * width,
            transcendentals=0,
        ),
    )(*lefts, right)


def scatter_sum(n_seq, partial, cover):
    nz = n_seq // 2
    seq = lax.axis_index("seq")
    z, y = seq // 2, lax.rem(seq, 2)
    rows = partial.shape[0] // n_seq
    pieces = partial.reshape(nz, 2, rows, partial.shape[1])
    away = lax.dynamic_index_in_dim(pieces, 1 - y, 1, keepdims=False)
    kept = lax.dynamic_index_in_dim(pieces, y, 1, keepdims=False)
    arrived = lax.ppermute(away, "seq", [(i, i ^ 1) for i in range(n_seq)])
    kept, *cover = lax.optimization_barrier((kept, *cover))
    summed = kept + arrived
    result = lax.dynamic_index_in_dim(summed, z, 0, keepdims=False)
    for k in range(1, nz):
        send = lax.dynamic_index_in_dim(summed, lax.rem(z + k, nz), 0, keepdims=False)
        result = result + lax.ppermute(
            send, "seq", [(i, (i + 2 * k) % n_seq) for i in range(n_seq)]
        )
    return result, cover


def solution(mesh):
    n_seq, n_tp = mesh.shape["seq"], mesh.shape["tp"]

    def per_device(inputs, out_grad, gate_weight, up_weight, down_weight):
        blocks, rows, width = inputs.shape
        x, dy, hidden, gate_unit, up_unit, partial = front(
            n_seq, n_tp,
            inputs.reshape(blocks * rows, width), out_grad.reshape(blocks * rows, width),
            gate_weight.T, up_weight.T, down_weight,
        )
        hidden_units = down_weight.shape[0]
        cover = weight_grads(hidden_units, (gate_unit, up_unit), x)
        total, (gate_grad, up_grad) = scatter_sum(n_seq, partial, cover)
        (down_grad,) = weight_grads(hidden_units, (hidden,), dy)
        return total.astype(BF16).reshape(inputs.shape), gate_grad.T, up_grad.T, down_grad

    return jax.shard_map(
        per_device,
        mesh=mesh,
        in_specs=(
            P(None, "seq", "tp"),
            P(None, "seq", "tp"),
            P("tp", "seq"),
            P("tp", "seq"),
            P("seq", "tp"),
        ),
        out_specs=(P(None, "seq", "tp"), P("tp", "seq"), P("tp", "seq"), P("seq", "tp")),
        check_vma=False,
    )
```
